32 devices in a mesh: dp: 8 (over y, x, core), mp: 4 (over z).
Axes of the slice: x: 2, y: 2, z: 4, core: 2. Of those that a mesh axis runs over, the one named last changes fastest.
Arguments:
- candidates: bfloat16 [64, 256, 768], P('dp', 'mp'), may hold values from -6 to 6
- owner_row: int32 [64], replicated, may hold values from 0 to 63, as said below
- selected: int32 [16], replicated, may hold values from 0 to 63, as said below
- dest_slot: int32 [16], replicated, may hold values from 0 to 15, as said below
- patch_weight: bfloat16 [768, 768], P(None, 'mp'), may hold values from -0.21875 to 0.21875
- positions: bfloat16 [256, 768], P(None, 'mp'), may hold values from -3 to 3
- qkv_weight: bfloat16 [768, 3, 768], P(None, None, 'mp'), may hold values from -1 to 1
- out_weight: bfloat16 [768, 768], P('mp'), may hold values from -0.21875 to 0.21875
- attn_gain: bfloat16 [768], replicated, may hold values from 0.099609375 to 1.8984375
- mlp_gain: bfloat16 [768], replicated, may hold values from 0.099609375 to 1.8984375
- up_weight: bfloat16 [768, 3072], P(None, 'mp'), may hold values from -0.21875 to 0.21875
- down_weight: bfloat16 [3072, 768], P('mp'), may hold values from -0.109375 to 0.109375
Outputs:
- layer_out: bfloat16 [16, 256, 768], P('dp', 'mp')
The draws below stay inside these ranges and needn't reach their ends.
Inputs may be any that keep to these rules, and one draw needn't show every extreme that they name: `owner_row`: a permutation; storage row r sits on index r // 8 of dp. `selected`: distinct candidates; no index of dp stores more than 4 of them, and some index stores exactly 4. `dest_slot`: a permutation; the 2 slots s with equal s // 2 get candidates stored on different indices of dp.
All inputs are finite; a program needn't handle non-finite values.
Results may differ from the reference program's by a relative error of at most 0.012.
Values may be sent and summed in bfloat16 or wider, within the bound.
A program may use at most 128 MiB of HBM per device.

```python
import math
import jax
import jax.numpy as jnp
from jax import lax

D = 768
HEADS = 12
FF = 3072
PIX = 768
PATCHES = 256
CAND_DEV = 8
SEL_DEV = 2
MOST = 4
HEAD_DIM = 64
CANDS = 64
SEL = 16
N_MP = 4


def routing_plan(key):
    subkeys = jax.random.split(jax.random.fold_in(key, 41), 5)
    learners = SEL // SEL_DEV
    owner_row = jax.random.permutation(subkeys[0], CANDS).astype(jnp.int32)
    placing = jax.random.permutation(subkeys[1], learners).astype(jnp.int32)
    position = jnp.argsort(placing).astype(jnp.int32)
    group_index = position // MOST
    within = position % MOST
    counts = jnp.where(group_index % 2 == 0, jnp.where(within < SEL_DEV, MOST, 0), SEL_DEV).astype(jnp.int32)
    run_end = jnp.cumsum(counts).astype(jnp.int32)
    starts = run_end - counts
    series = jnp.arange(SEL, dtype=jnp.int32)
    owners = jnp.sum((run_end[None, :] <= series[:, None]).astype(jnp.int32), axis=1).astype(jnp.int32)
    local_rank = series - starts[owners]
    shuffles = jax.vmap(lambda sub: jax.random.permutation(sub, CAND_DEV))(jax.random.split(subkeys[2], learners)).astype(jnp.int32)
    storage = owners * CAND_DEV + shuffles[owners, local_rank]
    inverse = jnp.argsort(owner_row).astype(jnp.int32)
    chosen = inverse[storage]
    learner_order = jax.random.permutation(subkeys[3], learners).astype(jnp.int32)
    slot_index = learner_order[series % learners] * SEL_DEV + series // learners
    mixing = jax.random.permutation(subkeys[4], SEL).astype(jnp.int32)
    return (owner_row, chosen[mixing].astype(jnp.int32), slot_index[mixing].astype(jnp.int32))


def draw_owner_row(key, part):
    return routing_plan(key)[0]


def draw_selected(key, part):
    return routing_plan(key)[1]


def draw_dest_slot(key, part):
    return routing_plan(key)[2]


def draw_qkv_weight(key, part):
    base = jax.random.normal(key, (D, 3, D), jnp.float32) / math.sqrt(D)
    return jnp.clip(base, -1.0, 1.0).astype(jnp.bfloat16)


def level_of(stream_key, dims, shards, least, high):
    loudness = 1.0
    for axis_at, shards_of in shards:
        steps = jax.random.uniform(jax.random.fold_in(jax.random.fold_in(stream_key, 6), axis_at), (shards_of,), jnp.float32, least / len(shards), high / len(shards))
        loudness = loudness * jnp.repeat(jnp.exp(steps), dims[axis_at] // shards_of).reshape((-1,) + (1,) * (len(dims) - 1 - axis_at))
    return loudness


def normal_values(own_key, shape, scale, most, cuts=(), held_as=jnp.bfloat16):
    result = jax.random.normal(own_key, shape, jnp.float32) * scale
    if len(cuts) > 0:
        result = level_of(own_key, shape, cuts, -0.22, 0.18) * result
    return jnp.clip(result, min=-most, max=most).astype(held_as)


def setup_inputs(seed: int = 0) -> dict:
    key_of = jax.random.split(jax.random.key(seed), 13)
    return {
        "candidates": normal_values(key_of[0], (CANDS, PATCHES, PIX), 1.0, 6.0, ((0, 8), (1, 4))),
        "owner_row": draw_owner_row(jax.random.fold_in(key_of[12], 71), 0),
        "selected": draw_selected(jax.random.fold_in(key_of[12], 71), 0),
        "dest_slot": draw_dest_slot(jax.random.fold_in(key_of[12], 71), 0),
        "patch_weight": normal_values(key_of[4], (PIX, D), PIX ** -0.5, 0.21875, ((1, 4),)),
        "positions": normal_values(key_of[5], (PATCHES, D), 0.5, 3.0, ((1, 4),)),
        "qkv_weight": draw_qkv_weight(jax.random.fold_in(key_of[12], 71), 0),
        "out_weight": normal_values(key_of[7], (D, D), D ** -0.5, 0.21875, ((0, 4),)),
        "attn_gain": jnp.clip(1.0 + 0.18 * jax.random.normal(key_of[8], (D,), jnp.float32), 0.099609375, 1.8984375).astype(jnp.bfloat16),
        "mlp_gain": jnp.clip(1.0 + 0.18 * jax.random.normal(key_of[9], (D,), jnp.float32), 0.099609375, 1.8984375).astype(jnp.bfloat16),
        "up_weight": normal_values(key_of[10], (D, FF), D ** -0.5, 0.21875, ((1, 4),)),
        "down_weight": normal_values(key_of[11], (FF, D), FF ** -0.5, 0.109375, ((0, 4),)),
    }


def norm_rows(values, gain):
    average = lax.optimization_barrier(jnp.mean(values, axis=-1, keepdims=True))
    centred = values - average
    variance = lax.optimization_barrier(jnp.mean(centred * centred, axis=-1, keepdims=True))
    return centred * lax.rsqrt(variance + 1e-06) * gain.astype(jnp.float32)

def group_sum(left, right, groups):
    count = left.shape[0]
    left_groups = left.reshape(count, groups, left.shape[1] // groups).astype(jnp.float32)
    right_groups = right.reshape(groups, right.shape[0] // groups, right.shape[1]).astype(jnp.float32)
    partials = jnp.einsum('tgk,gkd->tgd', left_groups, right_groups)
    rounded = lax.optimization_barrier(partials.astype(jnp.bfloat16))
    return lax.optimization_barrier(jnp.sum(rounded.astype(jnp.float32), axis=1))

def layer_one(pixels, patch_weight, positions, qkv_weight, out_weight, attn_gain, mlp_gain, up_weight, down_weight):
    embedded = (jnp.dot(pixels, patch_weight, preferred_element_type=jnp.float32) + positions.astype(jnp.float32)).astype(jnp.bfloat16)
    activations = embedded.astype(jnp.float32)
    normed = norm_rows(activations, attn_gain).astype(jnp.bfloat16)
    projected = jnp.einsum('td,dce->tce', normed.astype(jnp.float32), qkv_weight.astype(jnp.float32)).astype(jnp.bfloat16)
    head_split = projected.reshape(PATCHES, 3, HEADS, HEAD_DIM).astype(jnp.float32)
    queries = head_split[:, 0]
    attn_keys = head_split[:, 1]
    attn_values = head_split[:, 2]
    scores = jnp.einsum('qhd,khd->hqk', queries, attn_keys) * HEAD_DIM ** (-0.5)
    attn_probs = jax.nn.softmax(scores, axis=-1).astype(jnp.bfloat16)
    context = jnp.einsum('hqk,khd->qhd', attn_probs.astype(jnp.float32), attn_values).astype(jnp.bfloat16)
    context = context.reshape(PATCHES, D)
    attended = group_sum(context, out_weight, N_MP)
    after_attn = activations + attended
    normed2 = norm_rows(after_attn, mlp_gain).astype(jnp.bfloat16)
    hidden = jax.nn.gelu(jnp.dot(normed2, up_weight, preferred_element_type=jnp.float32), approximate=False).astype(jnp.bfloat16)
    feed = group_sum(hidden, down_weight, N_MP)
    return (after_attn + feed).astype(jnp.bfloat16)

def reference(candidates, owner_row, selected, dest_slot, patch_weight, positions, qkv_weight, out_weight, attn_gain, mlp_gain, up_weight, down_weight):
    chosen_rows = jnp.take(owner_row, selected).astype(jnp.int32)
    slot_rows = jnp.zeros((SEL,), jnp.int32).at[dest_slot].set(chosen_rows)
    batch = jnp.take(candidates, slot_rows, axis=0)

    def one_example(pixels):
        return layer_one(pixels, patch_weight, positions, qkv_weight, out_weight, attn_gain, mlp_gain, up_weight, down_weight)
    return lax.map(one_example, batch)
```

```python
import functools

import jax
import jax.numpy as jnp
from jax import lax
from jax.experimental import pallas as pl
from jax.experimental.pallas import tpu as pltpu
from jax.sharding import PartitionSpec as P

HEAD_DIM = 64
LANES = 128
PARTS = 2
MESH = pl.DeviceIdType.MESH
scope = jax.named_scope


def norm_rows(values, gain):
    average = jnp.mean(values, axis=-1, keepdims=True)
    centred = values - average
    variance = jnp.mean(centred * centred, axis=-1, keepdims=True)
    return centred * lax.rsqrt(variance + 1e-06) * gain


def dot(a, b):
    return jnp.dot(a, b, preferred_element_type=jnp.float32)


def dot_t(a, b):
    return lax.dot_general(a, b, (((1,), (1,)), ((), ())), preferred_element_type=jnp.float32)


def kernel(
    n_dp, n_mp, stored, per,
    owner_row, selected, dest_slot,
    cand_h, pw, pos_t, gain1, gain2, qkv_h, out_h, up_h, down_h,
    out_hbm,
    cand, qkv, up, down, wrel, orel, posf,
    send, recv0, recv1, xr, n1, act, after, ctx, cx, n2, part, ra, rm, rb, out,
    route_s, route_r, wz_s, wz_r, wx_s, wx_r, wt_s, wt_r, oz_s, oz_r, ox_s, ox_r, ot_s, ot_r,
    ag_s, ag_r, cx_s, cx_r, rs_s, rs_r, loc,
):
    dp = lax.axis_index("dp")
    mp = lax.axis_index("mp")
    recvs = (recv0, recv1)
    quarter, width = cand.shape[1], cand.shape[2]
    feats = pw.shape[0]
    rows = quarter // PARTS
    tokens = n_mp * quarter
    group = wrel.shape[2] // LANES
    side = mp + 1 - 2 * lax.rem(mp, 2)
    across = lax.rem(mp + n_mp // 2, n_mp)
    corner = n_mp - 1 - mp
    rel = (mp, side, across, corner)
    twin = dp + 1 - 2 * lax.rem(dp, 2)
    place = lax.rem(dp, group)
    first = dp - place
    mates = group // 2 - 1

    barrier = pltpu.get_barrier_semaphore()
    for other in rel[1:]:
        pl.semaphore_signal(barrier, inc=1, device_id=(dp, other), device_id_type=MESH)

    @pl.loop(1, n_dp)
    def _(k):
        pl.semaphore_signal(barrier, inc=1, device_id=(lax.rem(dp + k, n_dp), mp), device_id_type=MESH)

    own_w = pltpu.make_async_copy(pw, wrel.at[0, :, pl.ds(0, width)], loc.at[0])
    own_p = pltpu.make_async_copy(pos_t, wrel.at[0, :, pl.ds(width, tokens)], loc.at[1])
    own_o = pltpu.make_async_copy(out_h, orel.at[0], loc.at[2])
    own_c = pltpu.make_async_copy(cand_h, cand, loc.at[3])
    for c in (own_w, own_p, own_c, own_o):
        c.start()
    later = [
        pltpu.make_async_copy(src, dst, loc.at[4 + j])
        for j, (src, dst) in enumerate(((qkv_h, qkv), (up_h, up), (down_h, down)))
    ]
    count = selected.shape[0]
    short = count <= 16

    def route(i):
        row = owner_row[selected[i]]
        slot = dest_slot[i]
        owner = lax.div(row, stored)
        return slot, owner, jnp.where(owner == dp, lax.div(slot, per), -1), lax.rem(row, stored)

    routes = [route(i) for i in range(count)] if short else []

    def choose(key, value, wanted):
        if short:
            found = jnp.int32(0)
            for entry in routes:
                found = jnp.where(entry[key] == wanted, entry[value], found)
            return found

        def body(i, found):
            entry = route(i)
            return jnp.where(entry[key] == wanted, entry[value], found)
        return lax.fori_loop(0, count, body, jnp.int32(0))

    def remote(src, dst, ss, rs, where):
        return pltpu.make_async_remote_copy(
            src_ref=src, dst_ref=dst, send_sem=ss, recv_sem=rs, device_id=where, device_id_type=MESH
        )

    def w_cut(j):
        return pl.ds(0, feats), pl.ds(pl.multiple_of(j * LANES, LANES), LANES)

    o_rows, o_cols = 2 * feats // group, width // 2

    def o_cut(j):
        return (
            pl.ds(pl.multiple_of(lax.div(j, 2) * o_rows, o_rows), o_rows),
            pl.ds(pl.multiple_of(lax.rem(j, 2) * o_cols, o_cols), o_cols),
        )

    unsent = []

    def go(c):
        c.start()
        unsent.append(c)
        return c

    class Spread:
        def __init__(self, buf, cut, zs, zr, xs, xr_, ts, tr):
            self.buf, self.cut = buf, cut
            self.zs, self.zr, self.xs, self.xr, self.ts, self.tr = zs, zr, xs, xr_, ts, tr

        def over_z(self):
            cut = self.cut(place)
            self.z = [
                go(remote(self.buf.at[(0, *cut)], self.buf.at[(r, *cut)], self.zs.at[r - 1], self.zr.at[r - 1], (dp, rel[r])))
                for r in (2, 3, 1)
            ]

        def block(self, j):
            return self.buf.at[(pl.ds(1, n_mp - 1), *self.cut(j))]

        def over_xy(self):
            for c in self.z:
                c.wait_recv()
            mine = self.block(place)
            self.x = []
            for k in range(1, mates + 1):
                peer = first + lax.rem(place + 2 * k, group)
                self.x.append(go(remote(mine, mine, self.xs.at[k - 1], self.xr.at[k - 1], (peer, mp))))
            self.t = [go(remote(mine, mine, self.ts.at[0], self.tr.at[0], (twin, mp)))]

        def to_twin(self, k):
            self.x[k - 1].wait_recv()
            got = self.block(lax.rem(place + group - 2 * k, group))
            self.t.append(go(remote(got, got, self.ts.at[k], self.tr.at[k], (twin, mp))))

        def end(self):
            for c in self.t:
                c.wait_recv()

    spread_w = Spread(wrel, w_cut, wz_s, wz_r, wx_s, wx_r, wt_s, wt_r)
    spread_o = Spread(orel, o_cut, oz_s, oz_r, ox_s, ox_r, ot_s, ot_r)

    for c in (own_w, own_p, own_c, own_o):
        c.wait()
    with scope("s_barrier"):
        pl.semaphore_wait(barrier, n_mp - 1 + n_dp - 1)

    with scope("s_pass"):
        spread_w.over_z()
        for h in range(PARTS):
            def pass_on(k):
                learner = lax.rem(dp + n_dp - k, n_dp)
                send[h, learner] = cand[choose(2, 3, learner), h * rows:(h + 1) * rows]
                remote(
                    send.at[h, learner], recvs[h].at[dp], route_s.at[h, learner], route_r.at[h, dp], (learner, mp)
                ).start()

            if short:
                for k in range(1, n_dp):
                    pass_on(k)
            else:
                pl.loop(1, n_dp)(pass_on)
            recvs[h][dp] = cand[choose(2, 3, dp), h * rows:(h + 1) * rows]
        spread_o.over_z()
        for c in later:
            c.start()
        senders = [choose(0, 1, dp * per + e) for e in range(per)]

    def gather_start(buf, base, e, h):
        at = 3 * (base + e * PARTS + h)
        return [
            go(remote(buf.at[e, h, 0], buf.at[e, h, r], ag_s.at[at + j], ag_r.at[at + j], (dp, rel[r])))
            for j, r in enumerate((2, 1))
        ]

    def gather_forward(buf, base, e, h, cs):
        at = 3 * (base + e * PARTS + h) + 2
        cs[0].wait_recv()
        cs.append(go(remote(buf.at[e, h, 2], buf.at[e, h, 3], ag_s.at[at], ag_r.at[at], (dp, side))))

    def gather_end(cs):
        cs[1].wait_recv()
        cs[2].wait_recv()

    every = range(per)
    halves = range(PARTS)
    gathers = {}
    with scope("s_wxy"):
        spread_w.over_xy()
    for h in halves:
        with scope("s_route"):
            @pl.loop(1, n_dp)
            def _(k):
                peer = lax.rem(dp + k, n_dp)
                remote(
                    send.at[h, peer], recvs[h].at[peer], route_s.at[h, peer], route_r.at[h, peer], (peer, mp)
                ).wait()

            for e in every:
                xr[e, h, 0] = recvs[h][senders[e]]
                gathers[e, h] = gather_start(xr, 0, e, h)
        if h == 0:
            with scope("s_oxy"):
                spread_o.over_xy()
    with scope("s_fwd1a"):
        for e in every:
            gather_forward(xr, 0, e, 0, gathers[e, 0])
    with scope("s_wtwin"):
        for k in range(1, mates + 1):
            spread_w.to_twin(k)
    with scope("s_fwd1b"):
        gather_forward(xr, 0, 0, 1, gathers[0, 1])
    with scope("s_wend"):
        spread_w.end()
    with scope("s_pos"):
        for q in range(n_mp):
            posf[:, q * feats:(q + 1) * feats] = jnp.transpose(wrel[rel[q], :, width:].astype(jnp.float32))

    g1 = gain1[...].astype(jnp.float32).reshape(1, width)
    g2 = gain2[...].astype(jnp.float32).reshape(1, width)

    def embed(e, h):
        w = jnp.concatenate([wrel[rel[q], :, :width] for q in range(n_mp)], axis=0)
        pos = jnp.concatenate(
            [posf[pl.ds(pl.multiple_of(rel[r] * quarter + h * rows, rows), rows)] for r in range(n_mp)], axis=0
        )
        prod = dot_t(xr[e, h].reshape(n_mp * rows, width), w)
        value = (prod + pos).astype(jnp.bfloat16).astype(jnp.float32)
        act[e, h] = value[:rows]
        n1[e, h * n_mp * rows:(h + 1) * n_mp * rows] = norm_rows(value, g1).astype(jnp.bfloat16)

    def attend(e):
        qkv_all = dot_t(n1[e], qkv[...].reshape(3 * feats, width)).astype(jnp.bfloat16)
        q = qkv_all[:, :feats] * jnp.bfloat16(HEAD_DIM ** (-0.5))
        k = qkv_all[:, feats:2 * feats]
        v = qkv_all[:, 2 * feats:]
        for head in range(feats // HEAD_DIM):
            cut = slice(head * HEAD_DIM, (head + 1) * HEAD_DIM)
            s = dot_t(q[:, cut], k[:, cut])
            p = jnp.exp(s - jnp.max(s, axis=-1, keepdims=True))
            total = jnp.sum(p, axis=-1, keepdims=True)
            c = (dot(p.astype(jnp.bfloat16), v[:, cut]) / total).astype(jnp.bfloat16)
            ctx[e, :, :, :, cut] = c.reshape(PARTS, n_mp, rows, HEAD_DIM)
        return [
            go(remote(ctx.at[e, :, r], cx.at[e, r - 1], cx_s.at[3 * e + r - 1], cx_r.at[3 * e + r - 1], (dp, rel[r])))
            for r in (3, 2, 1)
        ]

    def project(e, cs):
        for c in cs:
            c.wait_recv()
        total = dot(ctx[e, :, 0].reshape(quarter, feats), orel[0])
        for r in range(1, n_mp):
            total += dot(cx[e, r - 1].reshape(quarter, feats), orel[r])
        value = act[e].reshape(quarter, width) + total
        after[e] = value.reshape(PARTS, rows, width)
        normed = norm_rows(value, g2).astype(jnp.bfloat16)
        for h in halves:
            n2[e, h, 0] = normed[h * rows:(h + 1) * rows]
            gathers[e, h] = gather_start(n2, per * PARTS, e, h)

    sums = {}

    def mlp(e, h):
        x = dot(n2[e, h].reshape(n_mp * rows, width), up[...])
        hidden = (0.5 * x * (1.0 + lax.erf(x * 0.7071067811865476))).astype(jnp.bfloat16)
        part[e, h] = dot(hidden, down[...]).astype(jnp.bfloat16).reshape(n_mp, rows, width)
        at = 3 * (e * PARTS + h)
        sums[e, h] = [
            go(remote(part.at[e, h, r], ra.at[e, h, j], rs_s.at[at + j], rs_r.at[at + j], (dp, side)))
            for j, r in enumerate((3, 1))
        ]

    def merge(e, h):
        at = 3 * (e * PARTS + h) + 2
        sums[e, h][0].wait_recv()
        rm[e, h] = (part[e, h, 2].astype(jnp.float32) + ra[e, h, 0].astype(jnp.float32)).astype(jnp.bfloat16)
        sums[e, h].append(go(remote(rm.at[e, h], rb.at[e, h], rs_s.at[at], rs_r.at[at], (dp, across))))

    def finish(e, h):
        cs = sums[e, h]
        cs[1].wait_recv()
        cs[2].wait_recv()
        total = part[e, h, 0].astype(jnp.float32) + ra[e, h, 1].astype(jnp.float32) + rb[e, h].astype(jnp.float32)
        out[e, h] = (after[e, h] + total).astype(jnp.bfloat16)
        c = pltpu.make_async_copy(out.at[e, h], out_hbm.at[e, pl.ds(h * rows, rows)], loc.at[7 + e * PARTS + h])
        c.start()
        return c

    contexts = []
    for e in every:
        for h in halves:
            if (e, h) == (per - 1, PARTS - 1):
                with scope("s_fwd1c"):
                    gather_forward(xr, 0, e, h, gathers[e, h])
            with scope("s_ag1end"):
                gather_end(gathers[e, h])
            with scope("s_embed"):
                embed(e, h)
        if e == 0:
            with scope("s_otwin"):
                for k in range(1, mates + 1):
                    spread_o.to_twin(k)
                later[0].wait()
        else:
            with scope("s_proj0"):
                spread_o.end()
                project(e - 1, contexts[e - 1])
        with scope("s_attend"):
            contexts.append(attend(e))
    with scope("s_fwd2a"):
        for h in halves:
            gather_forward(n2, per * PARTS, 0, h, gathers[0, h])
    with scope("s_proj1"):
        project(per - 1, contexts[per - 1])
    for c in later[1:]:
        c.wait()
    for h in halves:
        with scope("s_ag2a"):
            gather_end(gathers[0, h])
        with scope("s_mlp"):
            mlp(0, h)
    for h in halves:
        with scope("s_fwd2b"):
            gather_forward(n2, per * PARTS, 1, h, gathers[1, h])
        with scope("s_merge0"):
            merge(0, h)
    for h in halves:
        with scope("s_ag2b"):
            gather_end(gathers[1, h])
        with scope("s_mlp"):
            mlp(1, h)
    outs = []
    with scope("s_fin0"):
        for h in halves:
            outs.append(finish(0, h))
    for h in halves:
        with scope("s_merge1"):
            merge(1, h)
    for h in halves:
        with scope("s_fin1"):
            outs.append(finish(1, h))
    with scope("s_drain"):
        for c in unsent:
            c.wait_send()
        for c in outs:
            c.wait()


def solution(mesh):
    n_dp, n_mp = mesh.shape["dp"], mesh.shape["mp"]

    def local(
        candidates, owner_row, selected, dest_slot, patch_weight, positions,
        qkv_weight, out_weight, attn_gain, mlp_gain, up_weight, down_weight,
    ):
        stored, quarter, width = candidates.shape
        per = selected.shape[0] // n_dp
        feats = patch_weight.shape[1]
        tokens = positions.shape[0]
        rows = quarter // PARTS
        group = (width + tokens) // LANES
        mates = group // 2 - 1
        qkv = jnp.transpose(qkv_weight, (1, 2, 0))
        vm = pl.BlockSpec(memory_space=pltpu.VMEM)
        hb = pl.BlockSpec(memory_space=pl.ANY)
        sm = pl.BlockSpec(memory_space=pltpu.SMEM)
        bf, f32 = jnp.bfloat16, jnp.float32
        dma = pltpu.SemaphoreType.DMA
        chunks = per * PARTS
        return pl.pallas_call(
            functools.partial(kernel, n_dp, n_mp, stored, per),
            out_shape=jax.ShapeDtypeStruct((per, quarter, width), bf),
            in_specs=[sm] * 3 + [hb] * 3 + [vm] * 2 + [hb] * 4,
            out_specs=hb,
            scratch_shapes=[
                pltpu.VMEM(candidates.shape, bf), pltpu.VMEM(qkv.shape, bf),
                pltpu.VMEM(up_weight.shape, bf), pltpu.VMEM(down_weight.shape, bf),
                pltpu.VMEM((n_mp, feats, width + tokens), bf),
                pltpu.VMEM((n_mp, feats, width), bf),
                pltpu.VMEM((tokens, width), f32),
                pltpu.VMEM((PARTS, n_dp, rows, width), bf),
                pltpu.VMEM((n_dp, rows, width), bf), pltpu.VMEM((n_dp, rows, width), bf),
                pltpu.VMEM((per, PARTS, n_mp, rows, width), bf),
                pltpu.VMEM((per, tokens, width), bf),
                pltpu.VMEM((per, PARTS, rows, width), f32),
                pltpu.VMEM((per, PARTS, rows, width), f32),
                pltpu.VMEM((per, PARTS, n_mp, rows, feats), bf),
                pltpu.VMEM((per, n_mp - 1, PARTS, rows, feats), bf),
                pltpu.VMEM((per, PARTS, n_mp, rows, width), bf),
                pltpu.VMEM((per, PARTS, n_mp, rows, width), bf),
                pltpu.VMEM((per, PARTS, 2, rows, width), bf),
                pltpu.VMEM((per, PARTS, rows, width), bf),
                pltpu.VMEM((per, PARTS, rows, width), bf),
                pltpu.VMEM((per, PARTS, rows, width), bf),
                dma((PARTS, n_dp)), dma((PARTS, n_dp)),
                dma((3,)), dma((3,)), dma((mates,)), dma((mates,)), dma((mates + 1,)), dma((mates + 1,)),
                dma((3,)), dma((3,)), dma((mates,)), dma((mates,)), dma((mates + 1,)), dma((mates + 1,)),
                dma((6 * chunks,)), dma((6 * chunks,)),
                dma((3 * per,)), dma((3 * per,)),
                dma((3 * chunks,)), dma((3 * chunks,)),
                dma((7 + chunks,)),
            ],
            compiler_params=pltpu.CompilerParams(
                collective_id=0, has_side_effects=True, vmem_limit_bytes=60 * 1024 * 1024
            ),
        )(
            owner_row, selected, dest_slot, candidates, patch_weight.T, positions.T,
            attn_gain, mlp_gain, qkv, out_weight, up_weight, down_weight,
        )

    return jax.shard_map(
        local,
        mesh=mesh,
        in_specs=(
            P("dp", "mp", None), P(), P(), P(), P(None, "mp"), P(None, "mp"), P(None, None, "mp"),
            P("mp", None), P(), P(), P(None, "mp"), P("mp", None),
        ),
        out_specs=P("dp", "mp", None),
        check_vma=False,
    )
```

```python
import functools

import jax
import jax.numpy as jnp
from jax import lax
from jax.experimental import pallas as pl
from jax.experimental.pallas import tpu as pltpu
from jax.sharding import PartitionSpec as P

HEAD_DIM = 64
LANES = 128
PARTS = 2
MESH = pl.DeviceIdType.MESH
scope = jax.named_scope


def norm_rows(values, gain):
    average = jnp.mean(values, axis=-1, keepdims=True)
    centred = values - average
    variance = jnp.mean(centred * centred, axis=-1, keepdims=True)
    return centred * lax.rsqrt(variance + 1e-06) * gain


def dot(a, b):
    return jnp.dot(a, b, preferred_element_type=jnp.float32)


def dot_t(a, b):
    return lax.dot_general(a, b, (((1,), (1,)), ((), ())), preferred_element_type=jnp.float32)


def kernel(
    n_dp, n_mp, stored, per,
    owner_h, selected_h, dest_h,
    cand_h, pw, pos_t, gain1_h, gain2_h, qkv_h, out_h, up_h, down_h,
    out_hbm,
    owner_row, selected, dest_slot, gain1, gain2,
    cand, qkv, up, down, up2, down2, wrel, orel, posf,
    send, recv0, recv1, xr, n1, act, after, ctx, cx, n2, hid, part, ra, out,
    route_s, route_r, ws, wr, os_, or_, us, ur, ds_, dr, ag_s, ag_r, cx_s, cx_r, tk_s, tk_r, rs_s, rs_r, loc,
):
    dp = lax.axis_index("dp")
    mp = lax.axis_index("mp")
    recvs = (recv0, recv1)
    quarter, width = cand.shape[1], cand.shape[2]
    feats = pw.shape[0]
    rows = quarter // PARTS
    tokens = n_mp * quarter
    group = wrel.shape[2] // LANES
    side = mp + 1 - 2 * lax.rem(mp, 2)
    across = lax.rem(mp + n_mp // 2, n_mp)
    corner = n_mp - 1 - mp
    rel = (mp, side, across, corner)
    inner = (mp > 0) & (mp < n_mp - 1)
    outer = jnp.logical_not(inner)
    twin = dp + 1 - 2 * lax.rem(dp, 2)
    place = lax.rem(dp, group)
    first = dp - place

    barrier = pltpu.get_barrier_semaphore()
    for other in rel[1:]:
        pl.semaphore_signal(barrier, inc=1, device_id=(dp, other), device_id_type=MESH)

    @pl.loop(1, n_dp)
    def _(k):
        pl.semaphore_signal(barrier, inc=1, device_id=(lax.rem(dp + k, n_dp), mp), device_id_type=MESH)

    own_w = pltpu.make_async_copy(pw, wrel.at[0, :, pl.ds(0, width)], loc.at[0])
    own_p = pltpu.make_async_copy(pos_t, wrel.at[0, :, pl.ds(width, tokens)], loc.at[1])
    own_o = pltpu.make_async_copy(out_h, orel.at[0], loc.at[2])
    own_c = pltpu.make_async_copy(cand_h, cand, loc.at[3])
    tables = [
        pltpu.make_async_copy(src, dst, loc.at[7 + j])
        for j, (src, dst) in enumerate(
            ((owner_h, owner_row), (selected_h, selected), (dest_h, dest_slot), (gain1_h, gain1), (gain2_h, gain2))
        )
    ]
    for c in (*tables, own_c, own_w, own_p, own_o):
        c.start()
    later = [
        pltpu.make_async_copy(src, dst, loc.at[4 + j])
        for j, (src, dst) in enumerate(((qkv_h, qkv), (up_h, up), (down_h, down)))
    ]
    count = selected.shape[0]
    short = count <= 16

    def route(i):
        row = owner_row[selected[i]]
        slot = dest_slot[i]
        owner = lax.div(row, stored)
        return slot, owner, jnp.where(owner == dp, lax.div(slot, per), -1), lax.rem(row, stored)

    for c in tables:
        c.wait()
    routes = [route(i) for i in range(count)] if short else []

    def choose(key, value, wanted):
        if short:
            found = jnp.int32(0)
            for entry in routes:
                found = jnp.where(entry[key] == wanted, entry[value], found)
            return found

        def body(i, found):
            entry = route(i)
            return jnp.where(entry[key] == wanted, entry[value], found)
        return lax.fori_loop(0, count, body, jnp.int32(0))

    def remote(src, dst, ss, rs, where):
        return pltpu.make_async_remote_copy(
            src_ref=src, dst_ref=dst, send_sem=ss, recv_sem=rs, device_id=where, device_id_type=MESH
        )

    def flip(index, bit):
        return index + bit - 2 * bit * lax.rem(lax.div(index, bit), 2)

    def w_cut(j):
        return pl.ds(0, feats), pl.ds(pl.multiple_of(j * LANES, LANES), LANES)

    o_rows, o_cols = 2 * feats // group, width // 2

    def o_cut(j):
        return (
            pl.ds(pl.multiple_of(lax.div(j, 2) * o_rows, o_rows), o_rows),
            pl.ds(pl.multiple_of(lax.rem(j, 2) * o_cols, o_cols), o_cols),
        )

    core = lax.rem(place, 2)
    along_x, along_y = flip(place, 2), flip(place, 4)
    peers = (
        along_y + core * (along_x - along_y), along_x + core * (along_y - along_x), flip(along_x, 4)
    )
    homes = [first + peer for peer in peers]

    def landed(ref, sem):
        remote(ref, ref, sem, sem, (twin, mp)).wait_recv()

    def left(ref, sem):
        remote(ref, ref, sem, sem, (twin, mp)).wait_send()

    class Spread:
        def __init__(self, buf, cut, several, ss, rs, lead):
            self.buf, self.cut, self.several, self.ss, self.rs, self.lead = buf, cut, several, ss, rs, lead

        def block(self, j):
            return self.buf.at[(*self.lead, *self.cut(j))]

        def group(self, n):
            return self.buf.at[(*self.lead, *self.several(n))]

        def over_xy(self, direct=False):
            mine = self.block(place)
            for k in (2, 0, 1) if direct else (0, 1):
                remote(mine, mine, self.ss.at[1], self.rs.at[min(1 + k, 2)], (homes[k], mp)).start()
            remote(mine, mine, self.ss.at[2], self.rs.at[3], (twin, mp)).start()

        def to_twin(self, j):
            got = self.block(j)
            remote(got, got, self.ss.at[2], self.rs.at[3], (twin, mp)).start()

        def relay(self):
            got = self.block(peers[0])
            landed(got, self.rs.at[1])
            remote(got, got, self.ss.at[1], self.rs.at[2], (homes[1], mp)).start()
            self.to_twin(peers[0])

        def near(self):
            landed(self.block(peers[0]), self.rs.at[1])
            self.to_twin(peers[0])

        def rest(self):
            landed(self.group(2), self.rs.at[2])
            self.to_twin(peers[1])
            self.to_twin(peers[2])

        def end(self):
            landed(self.group(4), self.rs.at[3])

        def drain(self):
            left(self.group(3), self.ss.at[1])
            left(self.group(4), self.ss.at[2])

    class Planes(Spread):
        def over_z(self):
            cut = self.cut(place)
            for r in (2, 3, 1):
                remote(
                    self.buf.at[(0, *cut)], self.buf.at[(r, *cut)], self.ss.at[0], self.rs.at[0], (dp, rel[r])
                ).start()

        def from_z(self):
            landed(self.block(place), self.rs.at[0])

        def z_left(self, n):
            left(self.block(place), self.ss.at[0])

    class Lend(Spread):
        def over_z(self, src):
            rows_ = self.cut(place)
            remote(src.at[rows_], self.buf.at[rows_], self.ss.at[0], self.rs.at[0], (dp, side)).start()

        def from_z(self):
            landed(self.block(place), self.rs.at[0])

    class Inner(Planes):
        def over_z(self):
            cut = self.cut(place)

            def send_to(r):
                remote(
                    self.buf.at[(0, *cut)], self.buf.at[(r, *cut)], self.ss.at[0], self.rs.at[0], (dp, rel[r])
                ).start()

            @pl.when(outer)
            def _():
                send_to(2)
                send_to(1)

            @pl.when(inner)
            def _():
                send_to(3)

        def z_left(self, n):
            cut = self.cut(place)
            left(self.buf.at[(pl.ds(0, n), *cut)], self.ss.at[0])

    def w_several(n):
        return pl.ds(0, feats), pl.ds(0, n * LANES)

    def o_several(n):
        return pl.ds(0, n * o_rows), pl.ds(0, o_cols)

    l_rows = up.shape[0] // group

    def l_cut(j):
        return (pl.ds(pl.multiple_of(j * l_rows, l_rows), l_rows),)

    def l_several(n):
        return (pl.ds(0, n * l_rows),)

    others = (pl.ds(1, n_mp - 1),)
    spread_w = Planes(wrel, w_cut, w_several, ws, wr, others)
    spread_o = Inner(orel, o_cut, o_several, os_, or_, others)
    lend_up = Lend(up2, l_cut, l_several, us, ur, ())
    lend_down = Lend(down2, l_cut, l_several, ds_, dr, ())

    for c in (own_w, own_p, own_c, own_o):
        c.wait()
    with scope("s_barrier"):
        pl.semaphore_wait(barrier, n_mp - 1 + n_dp - 1)

    with scope("s_pass"):
        spread_w.over_z()

        @pl.when(outer)
        def _():
            lend_up.over_z(up_h)
        spread_o.over_z()
        learners = []
        if short:
            learners = [lax.rem(dp + k, n_dp) for k in range(1, n_dp)]
        if n_dp == group:
            learners = [flip(home, b) if b else home for home in homes[::-1] for b in (0, 1)] + [twin]
        for h in range(PARTS):
            def pass_on(k):
                learner = k if short else lax.rem(dp + n_dp - k, n_dp)
                send[h, learner] = cand[choose(2, 3, learner), h * rows:(h + 1) * rows]
                remote(
                    send.at[h, learner], recvs[h].at[dp], route_s.at[h], route_r.at[h], (learner, mp)
                ).start()

            if short:
                for learner in learners:
                    pass_on(learner)
            else:
                pl.loop(1, n_dp)(pass_on)
            recvs[h][dp] = cand[choose(2, 3, dp), h * rows:(h + 1) * rows]
        for c in later:
            c.start()
        senders = [choose(0, 1, dp * per + e) for e in range(per)]

    every = range(per)
    halves = range(PARTS)
    chunks = [(e, h) for h in halves for e in every]

    def copy(src, dst, ss, rs, where):
        remote(src, dst, ss, rs, where).start()

    def gather_send(e, h, src, r, where):
        at = 3 * (e * PARTS + h) + r - 1
        copy(xr.at[e, h, src], xr.at[e, h, r], ag_s.at[0], ag_r.at[at], (dp, where))

    def gather_land(e, h, r):
        landed(xr.at[e, h, r], ag_r.at[3 * (e * PARTS + h) + r - 1])

    def gather_start(e, h):
        @pl.when(outer)
        def _():
            gather_send(e, h, 0, 2, across)

        @pl.when(inner)
        def _():
            gather_send(e, h, 0, 3, corner)
        gather_send(e, h, 0, 1, side)

    def gather_forward(e, h):
        @pl.when(inner)
        def _():
            gather_land(e, h, 3)
            gather_send(e, h, 3, 2, side)
            gather_land(e, h, 2)
            gather_send(e, h, 2, 3, side)

    def gather_end(e, h):
        @pl.when(outer)
        def _():
            gather_land(e, h, 2)
            gather_land(e, h, 3)
        gather_land(e, h, 1)

    def take(h):
        landed(recvs[h].at[pl.ds(0, n_dp - 1)], route_r.at[h])
        for e in every:
            xr[e, h, 0] = recvs[h][senders[e]]
            gather_start(e, h)

    def on_inner(name, *calls):
        with scope(name):
            @pl.when(inner)
            def _():
                for call in calls:
                    call()

    with scope("s_route0"):
        take(0)
    with scope("s_wxy"):
        spread_w.from_z()
        spread_w.over_xy()
    with scope("s_route1"):
        take(1)

        @pl.when(outer)
        def _():
            lend_down.over_z(down_h)
    with scope("s_wrelay"):
        spread_w.relay()
    for e in every:
        with scope("s_fwd1a"):
            gather_forward(e, 0)
    on_inner("s_oxy", spread_o.from_z, spread_o.over_xy)
    with scope("s_fwd1b"):
        gather_forward(0, PARTS - 1)
    with scope("s_wrest"):
        spread_w.rest()
    with scope("s_fwd1b"):
        gather_forward(1, PARTS - 1)
    on_inner("s_upxy", lend_up.from_z, lend_up.over_xy)
    with scope("s_wend"):
        spread_w.end()
    with scope("s_pos"):
        for q in range(n_mp):
            posf[:, q * feats:(q + 1) * feats] = jnp.transpose(wrel[rel[q], :, width:].astype(jnp.float32))

    g1 = gain1[...].astype(jnp.float32).reshape(1, width)
    g2 = gain2[...].astype(jnp.float32).reshape(1, width)

    def embed(those, h):
        w = jnp.concatenate([wrel[rel[q], :, :width] for q in range(n_mp)], axis=0)
        pos = jnp.concatenate(
            [posf[pl.ds(pl.multiple_of(rel[r] * quarter + h * rows, rows), rows)] for r in range(n_mp)], axis=0
        )
        size = n_mp * rows
        x = jnp.concatenate([xr[e, h].reshape(size, width) for e in those], axis=0)
        prod = dot_t(x, w)
        for j, e in enumerate(those):
            value = (prod[j * size:(j + 1) * size] + pos).astype(jnp.bfloat16).astype(jnp.float32)
            act[e, h] = value[:2 * rows].reshape(2, rows, width)
            n1[e, h * size:(h + 1) * size] = norm_rows(value, g1).astype(jnp.bfloat16)

    def attend(e):
        qkv_all = dot_t(n1[e], qkv[...].reshape(3 * feats, width)).astype(jnp.bfloat16)
        q = qkv_all[:, :feats] * jnp.bfloat16(HEAD_DIM ** (-0.5))
        k = qkv_all[:, feats:2 * feats]
        v = qkv_all[:, 2 * feats:]
        for head in range(feats // HEAD_DIM):
            cut = slice(head * HEAD_DIM, (head + 1) * HEAD_DIM)
            s = dot_t(q[:, cut], k[:, cut])
            p = jnp.exp(s - jnp.max(s, axis=-1, keepdims=True))
            total = jnp.sum(p, axis=-1, keepdims=True)
            c = (dot(p.astype(jnp.bfloat16), v[:, cut]) / total).astype(jnp.bfloat16)
            c = c.reshape(PARTS, n_mp, rows, HEAD_DIM)
            for h in halves:
                at = h * feats + head * HEAD_DIM
                ctx[e, :, :, at:at + HEAD_DIM] = c[h]
        def send_to(r, at, b, where):
            copy(ctx.at[e, r], cx.at[e, at, b], cx_s.at[0], cx_r.at[e], (dp, where))

        @pl.when(outer)
        def _():
            for r in (2, 3):
                send_to(r, 1, r - 2, across)
            for r in (0, 1):
                send_to(r, 0, 1 - r, side)

        @pl.when(inner)
        def _():
            for r in (3, 2):
                send_to(r, 2, 3 - r, corner)

    def context_land(e):
        landed(cx.at[e], cx_r.at[e])

    def project(e):
        total = jnp.zeros((2 * quarter, width), jnp.float32)
        for r in range(n_mp):
            packed = [ctx[e, b] if r == 0 else cx[e, r - 1, b] for b in range(2)]
            block = jnp.concatenate(
                [packed[b][:, h * feats:(h + 1) * feats] for h in halves for b in range(2)], axis=0
            )
            total += dot(block, orel[r])
        value = act[e].reshape(2 * quarter, width) + total
        after[e] = value.reshape(PARTS, 2, rows, width)
        normed = norm_rows(value, g2).astype(jnp.bfloat16).reshape(PARTS, 2, rows, width)
        for h in halves:
            at = tk_r.at[e * PARTS + h]
            for b in range(2):
                n2[e, h, b] = normed[h, b]
                copy(n2.at[e, h, b], n2.at[e, h, 3 - b], tk_s.at[0], at, (dp, corner))

    def mlp_up(e, h):
        landed(n2.at[e, h, pl.ds(2, 2)], tk_r.at[e * PARTS + h])
        x = n2[e, h].reshape(n_mp * rows, width)
        for j, u in enumerate((up, up2)):
            y = dot(x, u[...])
            hid[e, h, j] = (0.5 * y * (1.0 + lax.erf(y * 0.7071067811865476))).astype(jnp.bfloat16)

    def mlp_down(e, h):
        total = dot(hid[e, h, 0], down[...]) + dot(hid[e, h, 1], down2[...])
        total = total.reshape(n_mp, rows, width)
        for r in (2, 3, 1, 0):
            part[e, h, r] = (total[r] + after[e, h, r] if r < 2 else total[r]).astype(jnp.bfloat16)
        for r in (2, 3, 1):
            copy(part.at[e, h, r], ra.at[e, h, int(r > 1)], rs_s.at[0], rs_r.at[e * PARTS + h], (dp, rel[r]))

    def finish(e, h, mine):
        got = pl.ds(0, 2) if mine is None else pl.ds(1, 1)
        landed(ra.at[e, h, got], rs_r.at[e * PARTS + h])
        total = (ra[e, h, 0] if mine is None else mine[e, h, 0]).astype(jnp.float32) + ra[e, h, 1].astype(jnp.float32)
        out[e, h] = total.astype(jnp.bfloat16)
        pltpu.make_async_copy(out.at[e, h], out_hbm.at[e, pl.ds(h * rows, rows)], loc.at[0]).start()

    with scope("s_ag1end"):
        for e in every:
            gather_end(e, 0)
    with scope("s_embed"):
        embed(every, 0)
    for e in every:
        with scope("s_ag1end"):
            gather_end(e, 1)
        with scope("s_embed"):
            embed([e], 1)
        if e == 0:
            later[0].wait()
        with scope("s_attend"):
            attend(e)
        if e == 0:
            on_inner("s_orelay", spread_o.relay)
            on_inner("s_uprelay", lend_up.relay)
            on_inner("s_downxy", lend_down.from_z, lend_down.over_xy)
    on_inner("s_orest", spread_o.rest)
    on_inner("s_oend", spread_o.end)
    for e in every:
        on_inner("s_cwait", functools.partial(context_land, e))
        on_inner("s_proj", functools.partial(project, e))
        if e == 0:
            on_inner("s_downrelay", lend_down.relay)
    for c in later[1:]:
        c.wait()

    @pl.when(inner)
    def _():
        with scope("s_uprest"):
            lend_up.rest()
        with scope("s_downrest"):
            lend_down.rest()
        with scope("s_upend"):
            lend_up.end()
        with scope("s_downend"):
            lend_down.end()
        for e, h in [(e, h) for e in every for h in halves][0:]:
            with scope("s_mlpup"):
                mlp_up(e, h)
            with scope("s_mlp"):
                mlp_down(e, h)
        with scope("s_finish"):
            for e in every:
                for h in halves:
                    finish(e, h, part)

    @pl.when(outer)
    def _():
        with scope("s_finish"):
            for e in every:
                for h in halves:
                    finish(e, h, None)

    with scope("s_drain"):
        for h in halves:
            left(send.at[h, pl.ds(0, n_dp - 1)], route_s.at[h])
        spread_w.z_left(3)
        spread_w.drain()

        @pl.when(inner)
        def _():
            spread_o.z_left(1)
            spread_o.drain()
            lend_up.drain()
            lend_down.drain()
            left(xr, ag_s.at[0])
            left(ctx.at[0], cx_s.at[0])
            left(n2.at[0], tk_s.at[0])
            left(part.at[:, :, pl.ds(0, n_mp - 1)], rs_s.at[0])

        @pl.when(outer)
        def _():
            spread_o.z_left(2)
            left(lend_up.block(place), us.at[0])
            left(lend_down.block(place), ds_.at[0])
            left(xr.at[0], ag_s.at[0])
            left(ctx, cx_s.at[0])

        pltpu.make_async_copy(out, out, loc.at[0]).wait()


def solution(mesh):
    n_dp, n_mp = mesh.shape["dp"], mesh.shape["mp"]

    def local(
        candidates, owner_row, selected, dest_slot, patch_weight, positions,
        qkv_weight, out_weight, attn_gain, mlp_gain, up_weight, down_weight,
    ):
        stored, quarter, width = candidates.shape
        per = selected.shape[0] // n_dp
        feats = patch_weight.shape[1]
        tokens = positions.shape[0]
        rows = quarter // PARTS
        qkv = jnp.transpose(qkv_weight, (1, 2, 0))
        hb = pl.BlockSpec(memory_space=pl.ANY)
        bf, f32 = jnp.bfloat16, jnp.float32
        dma = pltpu.SemaphoreType.DMA
        chunks = per * PARTS
        return pl.pallas_call(
            functools.partial(kernel, n_dp, n_mp, stored, per),
            out_shape=jax.ShapeDtypeStruct((per, quarter, width), bf),
            in_specs=[hb] * 12,
            out_specs=hb,
            scratch_shapes=[
                *[pltpu.SMEM(x.shape, x.dtype) for x in (owner_row, selected, dest_slot)],
                pltpu.VMEM(attn_gain.shape, bf), pltpu.VMEM(mlp_gain.shape, bf),
                pltpu.VMEM(candidates.shape, bf), pltpu.VMEM(qkv.shape, bf),
                pltpu.VMEM(up_weight.shape, bf), pltpu.VMEM(down_weight.shape, bf),
                pltpu.VMEM(up_weight.shape, bf), pltpu.VMEM(down_weight.shape, bf),
                pltpu.VMEM((n_mp, feats, width + tokens), bf),
                pltpu.VMEM((n_mp, feats, width), bf),
                pltpu.VMEM((tokens, width), f32),
                pltpu.VMEM((PARTS, n_dp, rows, width), bf),
                pltpu.VMEM((n_dp, rows, width), bf), pltpu.VMEM((n_dp, rows, width), bf),
                pltpu.VMEM((per, PARTS, n_mp, rows, width), bf),
                pltpu.VMEM((per, tokens, width), bf),
                pltpu.VMEM((per, PARTS, 2, rows, width), f32),
                pltpu.VMEM((per, PARTS, 2, rows, width), f32),
                pltpu.VMEM((per, n_mp, rows, PARTS * feats), bf),
                pltpu.VMEM((per, n_mp - 1, 2, rows, PARTS * feats), bf),
                pltpu.VMEM((per, PARTS, n_mp, rows, width), bf),
                pltpu.VMEM((per, PARTS, 2, n_mp * rows, up_weight.shape[1]), bf),
                pltpu.VMEM((per, PARTS, n_mp, rows, width), bf),
                pltpu.VMEM((per, PARTS, 2, rows, width), bf),
                pltpu.VMEM((per, PARTS, rows, width), bf),
                *[dma((n,)) for n in (PARTS, PARTS, 3, 4, 3, 4, 3, 4, 3, 4)],
                *[dma((n,)) for n in (1, 3 * chunks, 1, per, 1, chunks, 1, chunks, 12)],
            ],
            compiler_params=pltpu.CompilerParams(
                collective_id=0, has_side_effects=True, vmem_limit_bytes=60 * 1024 * 1024
            ),
        )(
            owner_row, selected, dest_slot, candidates, patch_weight.T, positions.T,
            attn_gain, mlp_gain, qkv, out_weight, up_weight, down_weight,
        )

    return jax.shard_map(
        local,
        mesh=mesh,
        in_specs=(
            P("dp", "mp", None), P(), P(), P(), P(None, "mp"), P(None, "mp"), P(None, None, "mp"),
            P("mp", None), P(), P(), P(None, "mp"), P("mp", None),
        ),
        out_specs=P("dp", "mp", None),
        check_vma=False,
    )
```

```python
import functools

import jax
import jax.numpy as jnp
from jax import lax
from jax.experimental import pallas as pl
from jax.experimental.pallas import tpu as pltpu
from jax.sharding import PartitionSpec as P

HEAD_DIM = 64
LANES = 128
PARTS = 2
MESH = pl.DeviceIdType.MESH
scope = jax.named_scope


def norm_rows(values, gain):
    average = jnp.mean(values, axis=-1, keepdims=True)
    centred = values - average
    variance = jnp.mean(centred * centred, axis=-1, keepdims=True)
    return centred * lax.rsqrt(variance + 1e-06) * gain


def dot(a, b):
    return jnp.dot(a, b, preferred_element_type=jnp.float32)


def dot_t(a, b):
    return lax.dot_general(a, b, (((1,), (1,)), ((), ())), preferred_element_type=jnp.float32)


def kernel(
    n_dp, n_mp, stored, per,
    owner_h, selected_h, dest_h,
    cand_h, pw, pos_t, gain1_h, gain2_h, qkv_h, out_h, up_h, down_h,
    out_hbm,
    owner_row, selected, dest_slot, gain1, gain2,
    cand, qkv, up, down, up2, down2, wrel, orel, posf,
    send, recv0, recv1, xr, n1, act, after, ctx, cx, n2, hid, part, ra, out,
    route_s, route_r, ws, wr, os_, or_, us, ur, ds_, dr, ag_s, ag_r, cx_s, cx_r, tk_s, tk_r, rs_s, rs_r, loc,
):
    dp = lax.axis_index("dp")
    mp = lax.axis_index("mp")
    recvs = (recv0, recv1)
    quarter, width = cand.shape[1], cand.shape[2]
    feats = pw.shape[0]
    rows = quarter // PARTS
    tokens = n_mp * quarter
    group = wrel.shape[2] // LANES
    side = mp + 1 - 2 * lax.rem(mp, 2)
    across = lax.rem(mp + n_mp // 2, n_mp)
    corner = n_mp - 1 - mp
    rel = (mp, side, across, corner)
    inner = (mp > 0) & (mp < n_mp - 1)
    outer = jnp.logical_not(inner)
    twin = dp + 1 - 2 * lax.rem(dp, 2)
    place = lax.rem(dp, group)
    first = dp - place

    barrier = pltpu.get_barrier_semaphore()
    for other in rel[1:]:
        pl.semaphore_signal(barrier, inc=1, device_id=(dp, other), device_id_type=MESH)

    @pl.loop(1, n_dp)
    def _(k):
        pl.semaphore_signal(barrier, inc=1, device_id=(lax.rem(dp + k, n_dp), mp), device_id_type=MESH)

    own_w = pltpu.make_async_copy(pw, wrel.at[0, :, pl.ds(0, width)], loc.at[0])
    own_p = pltpu.make_async_copy(pos_t, wrel.at[0, :, pl.ds(width, tokens)], loc.at[1])
    own_o = pltpu.make_async_copy(out_h, orel.at[0], loc.at[2])
    own_c = pltpu.make_async_copy(cand_h, cand, loc.at[3])
    tables = [
        pltpu.make_async_copy(src, dst, loc.at[7 + j])
        for j, (src, dst) in enumerate(
            ((owner_h, owner_row), (selected_h, selected), (dest_h, dest_slot), (gain1_h, gain1), (gain2_h, gain2))
        )
    ]
    for c in (*tables, own_c, own_w, own_p, own_o):
        c.start()
    later = [
        pltpu.make_async_copy(src, dst, loc.at[4 + j])
        for j, (src, dst) in enumerate(((qkv_h, qkv), (up_h, up), (down_h, down)))
    ]
    count = selected.shape[0]
    short = count <= 16

    def route(i):
        row = owner_row[selected[i]]
        slot = dest_slot[i]
        owner = lax.div(row, stored)
        return slot, owner, jnp.where(owner == dp, lax.div(slot, per), -1), lax.rem(row, stored)

    for c in tables:
        c.wait()
    routes = [route(i) for i in range(count)] if short else []

    def choose(key, value, wanted):
        if short:
            found = jnp.int32(0)
            for entry in routes:
                found = jnp.where(entry[key] == wanted, entry[value], found)
            return found

        def body(i, found):
            entry = route(i)
            return jnp.where(entry[key] == wanted, entry[value], found)
        return lax.fori_loop(0, count, body, jnp.int32(0))

    def remote(src, dst, ss, rs, where):
        return pltpu.make_async_remote_copy(
            src_ref=src, dst_ref=dst, send_sem=ss, recv_sem=rs, device_id=where, device_id_type=MESH
        )

    def flip(index, bit):
        return index + bit - 2 * bit * lax.rem(lax.div(index, bit), 2)

    def w_cut(j):
        return pl.ds(0, feats), pl.ds(pl.multiple_of(j * LANES, LANES), LANES)

    o_rows, o_cols = 2 * feats // group, width // 2

    def o_cut(j):
        return (
            pl.ds(pl.multiple_of(lax.div(j, 2) * o_rows, o_rows), o_rows),
            pl.ds(pl.multiple_of(lax.rem(j, 2) * o_cols, o_cols), o_cols),
        )

    core = lax.rem(place, 2)
    along_x, along_y = flip(place, 2), flip(place, 4)
    peers = (
        along_y + core * (along_x - along_y), along_x + core * (along_y - along_x), flip(along_x, 4)
    )
    homes = [first + peer for peer in peers]

    def landed(ref, sem):
        remote(ref, ref, sem, sem, (twin, mp)).wait_recv()

    def left(ref, sem):
        remote(ref, ref, sem, sem, (twin, mp)).wait_send()

    class Spread:
        def __init__(self, buf, cut, several, ss, rs, lead):
            self.buf, self.cut, self.several, self.ss, self.rs, self.lead = buf, cut, several, ss, rs, lead

        def block(self, j):
            return self.buf.at[(*self.lead, *self.cut(j))]

        def group(self, n):
            return self.buf.at[(*self.lead, *self.several(n))]

        def over_xy(self, direct=False):
            mine = self.block(place)
            for k in (2, 0, 1) if direct else (0, 1):
                remote(mine, mine, self.ss.at[1], self.rs.at[min(1 + k, 2)], (homes[k], mp)).start()
            remote(mine, mine, self.ss.at[2], self.rs.at[3], (twin, mp)).start()

        def to_twin(self, j):
            got = self.block(j)
            remote(got, got, self.ss.at[2], self.rs.at[3], (twin, mp)).start()

        def relay(self):
            got = self.block(peers[0])
            landed(got, self.rs.at[1])
            remote(got, got, self.ss.at[1], self.rs.at[2], (homes[1], mp)).start()
            self.to_twin(peers[0])

        def near(self):
            landed(self.block(peers[0]), self.rs.at[1])
            self.to_twin(peers[0])

        def rest(self):
            landed(self.group(2), self.rs.at[2])
            self.to_twin(peers[1])
            self.to_twin(peers[2])

        def end(self):
            landed(self.group(4), self.rs.at[3])

        def drain(self):
            left(self.group(3), self.ss.at[1])
            left(self.group(4), self.ss.at[2])

    class Planes(Spread):
        def over_z(self):
            cut = self.cut(place)
            for r in (2, 3, 1):
                remote(
                    self.buf.at[(0, *cut)], self.buf.at[(r, *cut)], self.ss.at[0], self.rs.at[0], (dp, rel[r])
                ).start()

        def from_z(self):
            landed(self.block(place), self.rs.at[0])

        def z_left(self, n):
            left(self.block(place), self.ss.at[0])

    class Lend(Spread):
        def over_z(self, src):
            rows_ = self.cut(place)
            remote(src.at[rows_], self.buf.at[rows_], self.ss.at[0], self.rs.at[0], (dp, side)).start()

        def from_z(self):
            landed(self.block(place), self.rs.at[0])

    class Inner(Planes):
        def over_z(self):
            cut = self.cut(place)

            def send_to(r):
                remote(
                    self.buf.at[(0, *cut)], self.buf.at[(r, *cut)], self.ss.at[0], self.rs.at[0], (dp, rel[r])
                ).start()

            @pl.when(outer)
            def _():
                send_to(2)
                send_to(1)

            @pl.when(inner)
            def _():
                send_to(3)

        def z_left(self, n):
            cut = self.cut(place)
            left(self.buf.at[(pl.ds(0, n), *cut)], self.ss.at[0])

    def w_several(n):
        return pl.ds(0, feats), pl.ds(0, n * LANES)

    def o_several(n):
        return pl.ds(0, n * o_rows), pl.ds(0, o_cols)

    l_rows = up.shape[0] // group

    def l_cut(j):
        return (pl.ds(pl.multiple_of(j * l_rows, l_rows), l_rows),)

    def l_several(n):
        return (pl.ds(0, n * l_rows),)

    others = (pl.ds(1, n_mp - 1),)
    spread_w = Planes(wrel, w_cut, w_several, ws, wr, others)
    spread_o = Inner(orel, o_cut, o_several, os_, or_, others)
    lend_up = Lend(up2, l_cut, l_several, us, ur, ())
    lend_down = Lend(down2, l_cut, l_several, ds_, dr, ())

    for c in (own_w, own_p, own_c, own_o):
        c.wait()
    with scope("s_barrier"):
        pl.semaphore_wait(barrier, n_mp - 1 + n_dp - 1)

    with scope("s_pass"):
        spread_w.over_z()

        @pl.when(outer)
        def _():
            lend_up.over_z(up_h)
        spread_o.over_z()
        learners = []
        if short:
            learners = [lax.rem(dp + k, n_dp) for k in range(1, n_dp)]
        if n_dp == group:
            learners = [flip(home, b) if b else home for home in homes[::-1] for b in (0, 1)] + [twin]
        for h in range(PARTS):
            def pass_on(k):
                learner = k if short else lax.rem(dp + n_dp - k, n_dp)
                send[h, learner] = cand[choose(2, 3, learner), h * rows:(h + 1) * rows]
                remote(
                    send.at[h, learner], recvs[h].at[dp], route_s.at[h], route_r.at[h], (learner, mp)
                ).start()

            if short:
                for learner in learners:
                    pass_on(learner)
            else:
                pl.loop(1, n_dp)(pass_on)
            recvs[h][dp] = cand[choose(2, 3, dp), h * rows:(h + 1) * rows]
        for c in later:
            c.start()
        senders = [choose(0, 1, dp * per + e) for e in range(per)]

    every = range(per)
    halves = range(PARTS)
    chunks = [(e, h) for h in halves for e in every]

    def copy(src, dst, ss, rs, where):
        remote(src, dst, ss, rs, where).start()

    def gather_send(e, h, src, r, where):
        at = 3 * (e * PARTS + h) + r - 1
        copy(xr.at[e, h, src], xr.at[e, h, r], ag_s.at[0], ag_r.at[at], (dp, where))

    def gather_land(e, h, r):
        landed(xr.at[e, h, r], ag_r.at[3 * (e * PARTS + h) + r - 1])

    def gather_start(e, h):
        @pl.when(outer)
        def _():
            gather_send(e, h, 0, 2, across)

        @pl.when(inner)
        def _():
            gather_send(e, h, 0, 3, corner)
        gather_send(e, h, 0, 1, side)

    def gather_forward(e, h):
        @pl.when(inner)
        def _():
            gather_land(e, h, 3)
            gather_send(e, h, 3, 2, side)
            gather_land(e, h, 2)
            gather_send(e, h, 2, 3, side)

    def gather_end(e, h):
        @pl.when(outer)
        def _():
            gather_land(e, h, 2)
            gather_land(e, h, 3)
        gather_land(e, h, 1)

    def take(h):
        landed(recvs[h].at[pl.ds(0, n_dp - 1)], route_r.at[h])
        for e in every:
            xr[e, h, 0] = recvs[h][senders[e]]
            gather_start(e, h)

    def on_inner(name, *calls):
        with scope(name):
            @pl.when(inner)
            def _():
                for call in calls:
                    call()

    with scope("s_route0"):
        take(0)
    with scope("s_wxy"):
        spread_w.from_z()
        spread_w.over_xy()
    with scope("s_route1"):
        take(1)

        @pl.when(outer)
        def _():
            lend_down.over_z(down_h)
    with scope("s_wrelay"):
        spread_w.relay()
    for e in every:
        with scope("s_fwd1a"):
            gather_forward(e, 0)
    on_inner("s_oxy", spread_o.from_z, spread_o.over_xy)
    with scope("s_fwd1b"):
        gather_forward(0, PARTS - 1)
    with scope("s_wrest"):
        spread_w.rest()
    with scope("s_fwd1b"):
        gather_forward(1, PARTS - 1)
    on_inner("s_upxy", lend_up.from_z, lend_up.over_xy)
    with scope("s_wend"):
        spread_w.end()
    with scope("s_pos"):
        for q in range(n_mp):
            posf[:, q * feats:(q + 1) * feats] = jnp.transpose(wrel[rel[q], :, width:].astype(jnp.float32))

    g1 = gain1[...].astype(jnp.float32).reshape(1, width)
    g2 = gain2[...].astype(jnp.float32).reshape(1, width)

    def embed(those, h):
        w = jnp.concatenate([wrel[rel[q], :, :width] for q in range(n_mp)], axis=0)
        pos = jnp.concatenate(
            [posf[pl.ds(pl.multiple_of(rel[r] * quarter + h * rows, rows), rows)] for r in range(n_mp)], axis=0
        )
        size = n_mp * rows
        x = jnp.concatenate([xr[e, h].reshape(size, width) for e in those], axis=0)
        prod = dot_t(x, w)
        for j, e in enumerate(those):
            value = (prod[j * size:(j + 1) * size] + pos).astype(jnp.bfloat16).astype(jnp.float32)
            act[e, h] = value[:2 * rows].reshape(2, rows, width)
            n1[e, h * size:(h + 1) * size] = norm_rows(value, g1).astype(jnp.bfloat16)

    def attend(e):
        qkv_all = dot_t(n1[e], qkv[...].reshape(3 * feats, width)).astype(jnp.bfloat16)
        q = qkv_all[:, :feats] * jnp.bfloat16(HEAD_DIM ** (-0.5))
        k = qkv_all[:, feats:2 * feats]
        v = qkv_all[:, 2 * feats:]
        for head in range(feats // HEAD_DIM):
            cut = slice(head * HEAD_DIM, (head + 1) * HEAD_DIM)
            s = dot_t(q[:, cut], k[:, cut])
            p = jnp.exp(s - jnp.max(s, axis=-1, keepdims=True))
            total = jnp.sum(p, axis=-1, keepdims=True)
            c = (dot(p.astype(jnp.bfloat16), v[:, cut]) / total).astype(jnp.bfloat16)
            c = c.reshape(PARTS, n_mp, rows, HEAD_DIM)
            for h in halves:
                at = h * feats + head * HEAD_DIM
                ctx[e, :, :, at:at + HEAD_DIM] = c[h]
        def send_to(r, at, b, where):
            copy(ctx.at[e, r], cx.at[e, at, b], cx_s.at[0], cx_r.at[e], (dp, where))

        @pl.when(outer)
        def _():
            for r in (2, 3):
                send_to(r, 1, r - 2, across)
            for r in (0, 1):
                send_to(r, 0, 1 - r, side)

        @pl.when(inner)
        def _():
            for r in (3, 2):
                send_to(r, 2, 3 - r, corner)

    def context_land(e):
        landed(cx.at[e], cx_r.at[e])

    def project(e):
        total = jnp.zeros((2 * quarter, width), jnp.float32)
        for r in range(n_mp):
            packed = [ctx[e, b] if r == 0 else cx[e, r - 1, b] for b in range(2)]
            block = jnp.concatenate(
                [packed[b][:, h * feats:(h + 1) * feats] for h in halves for b in range(2)], axis=0
            )
            total += dot(block, orel[r])
        value = act[e].reshape(2 * quarter, width) + total
        after[e] = value.reshape(PARTS, 2, rows, width)
        normed = norm_rows(value, g2).astype(jnp.bfloat16).reshape(PARTS, 2, rows, width)
        for h in halves:
            at = tk_r.at[e * PARTS + h]
            for b in range(2):
                n2[e, h, b] = normed[h, b]
                copy(n2.at[e, h, b], n2.at[e, h, 3 - b], tk_s.at[0], at, (dp, corner))

    def mlp_up(e, h):
        landed(n2.at[e, h, pl.ds(2, 2)], tk_r.at[e * PARTS + h])
        x = n2[e, h].reshape(n_mp * rows, width)
        for j, u in enumerate((up, up2)):
            y = dot(x, u[...])
            hid[e, h, j] = (0.5 * y * (1.0 + lax.erf(y * 0.7071067811865476))).astype(jnp.bfloat16)

    def mlp_down(e, h):
        total = dot(hid[e, h, 0], down[...]) + dot(hid[e, h, 1], down2[...])
        total = total.reshape(n_mp, rows, width)
        for r in (2, 3, 1, 0):
            part[e, h, r] = (total[r] + after[e, h, r] if r < 2 else total[r]).astype(jnp.bfloat16)
        for r in (2, 3, 1):
            copy(part.at[e, h, r], ra.at[e, h, int(r > 1)], rs_s.at[0], rs_r.at[e * PARTS + h], (dp, rel[r]))

    def finish(e, h, mine):
        got = pl.ds(0, 2) if mine is None else pl.ds(1, 1)
        landed(ra.at[e, h, got], rs_r.at[e * PARTS + h])
        total = (ra[e, h, 0] if mine is None else mine[e, h, 0]).astype(jnp.float32) + ra[e, h, 1].astype(jnp.float32)
        out[e, h] = total.astype(jnp.bfloat16)
        pltpu.make_async_copy(out.at[e, h], out_hbm.at[e, pl.ds(h * rows, rows)], loc.at[0]).start()

    with scope("s_ag1end"):
        for e in every:
            gather_end(e, 0)
    with scope("s_embed"):
        embed(every, 0)
    for e in every:
        with scope("s_ag1end"):
            gather_end(e, 1)
        with scope("s_embed"):
            embed([e], 1)
        if e == 0:
            later[0].wait()
            on_inner("s_orelay", spread_o.relay)
            on_inner("s_downxy", lend_down.from_z, lend_down.over_xy)
        with scope("s_attend"):
            attend(e)
        if e == 0:
            on_inner("s_uprelay", lend_up.relay)
    on_inner("s_orest", spread_o.rest)
    on_inner("s_oend", spread_o.end)
    for e in every:
        on_inner("s_cwait", functools.partial(context_land, e))
        on_inner("s_proj", functools.partial(project, e))
        if e == 0:
            on_inner("s_downrelay", lend_down.relay)
    for c in later[1:]:
        c.wait()

    @pl.when(inner)
    def _():
        with scope("s_uprest"):
            lend_up.rest()
        with scope("s_downrest"):
            lend_down.rest()
        with scope("s_upend"):
            lend_up.end()
        with scope("s_downend"):
            lend_down.end()
        for e, h in [(e, h) for e in every for h in halves][0:]:
            with scope("s_mlpup"):
                mlp_up(e, h)
            with scope("s_mlp"):
                mlp_down(e, h)
        with scope("s_finish"):
            for e in every:
                for h in halves:
                    finish(e, h, part)

    @pl.when(outer)
    def _():
        with scope("s_finish"):
            for e in every:
                for h in halves:
                    finish(e, h, None)

    with scope("s_drain"):
        for h in halves:
            left(send.at[h, pl.ds(0, n_dp - 1)], route_s.at[h])
        spread_w.z_left(3)
        spread_w.drain()

        @pl.when(inner)
        def _():
            spread_o.z_left(1)
            spread_o.drain()
            lend_up.drain()
            lend_down.drain()
            left(xr, ag_s.at[0])
            left(ctx.at[0], cx_s.at[0])
            left(n2.at[0], tk_s.at[0])
            left(part.at[:, :, pl.ds(0, n_mp - 1)], rs_s.at[0])

        @pl.when(outer)
        def _():
            spread_o.z_left(2)
            left(lend_up.block(place), us.at[0])
            left(lend_down.block(place), ds_.at[0])
            left(xr.at[0], ag_s.at[0])
            left(ctx, cx_s.at[0])

        pltpu.make_async_copy(out, out, loc.at[0]).wait()


def solution(mesh):
    n_dp, n_mp = mesh.shape["dp"], mesh.shape["mp"]

    def local(
        candidates, owner_row, selected, dest_slot, patch_weight, positions,
        qkv_weight, out_weight, attn_gain, mlp_gain, up_weight, down_weight,
    ):
        stored, quarter, width = candidates.shape
        per = selected.shape[0] // n_dp
        feats = patch_weight.shape[1]
        tokens = positions.shape[0]
        rows = quarter // PARTS
        qkv = jnp.transpose(qkv_weight, (1, 2, 0))
        hb = pl.BlockSpec(memory_space=pl.ANY)
        bf, f32 = jnp.bfloat16, jnp.float32
        dma = pltpu.SemaphoreType.DMA
        chunks = per * PARTS
        return pl.pallas_call(
            functools.partial(kernel, n_dp, n_mp, stored, per),
            out_shape=jax.ShapeDtypeStruct((per, quarter, width), bf),
            in_specs=[hb] * 12,
            out_specs=hb,
            scratch_shapes=[
                *[pltpu.SMEM(x.shape, x.dtype) for x in (owner_row, selected, dest_slot)],
                pltpu.VMEM(attn_gain.shape, bf), pltpu.VMEM(mlp_gain.shape, bf),
                pltpu.VMEM(candidates.shape, bf), pltpu.VMEM(qkv.shape, bf),
                pltpu.VMEM(up_weight.shape, bf), pltpu.VMEM(down_weight.shape, bf),
                pltpu.VMEM(up_weight.shape, bf), pltpu.VMEM(down_weight.shape, bf),
                pltpu.VMEM((n_mp, feats, width + tokens), bf),
                pltpu.VMEM((n_mp, feats, width), bf),
                pltpu.VMEM((tokens, width), f32),
                pltpu.VMEM((PARTS, n_dp, rows, width), bf),
                pltpu.VMEM((n_dp, rows, width), bf), pltpu.VMEM((n_dp, rows, width), bf),
                pltpu.VMEM((per, PARTS, n_mp, rows, width), bf),
                pltpu.VMEM((per, tokens, width), bf),
                pltpu.VMEM((per, PARTS, 2, rows, width), f32),
                pltpu.VMEM((per, PARTS, 2, rows, width), f32),
                pltpu.VMEM((per, n_mp, rows, PARTS * feats), bf),
                pltpu.VMEM((per, n_mp - 1, 2, rows, PARTS * feats), bf),
                pltpu.VMEM((per, PARTS, n_mp, rows, width), bf),
                pltpu.VMEM((per, PARTS, 2, n_mp * rows, up_weight.shape[1]), bf),
                pltpu.VMEM((per, PARTS, n_mp, rows, width), bf),
                pltpu.VMEM((per, PARTS, 2, rows, width), bf),
                pltpu.VMEM((per, PARTS, rows, width), bf),
                *[dma((n,)) for n in (PARTS, PARTS, 3, 4, 3, 4, 3, 4, 3, 4)],
                *[dma((n,)) for n in (1, 3 * chunks, 1, per, 1, chunks, 1, chunks, 12)],
            ],
            compiler_params=pltpu.CompilerParams(
                collective_id=0, has_side_effects=True, vmem_limit_bytes=60 * 1024 * 1024
            ),
        )(
            owner_row, selected, dest_slot, candidates, patch_weight.T, positions.T,
            attn_gain, mlp_gain, qkv, out_weight, up_weight, down_weight,
        )

    return jax.shard_map(
        local,
        mesh=mesh,
        in_specs=(
            P("dp", "mp", None), P(), P(), P(), P(None, "mp"), P(None, "mp"), P(None, None, "mp"),
            P("mp", None), P(), P(), P(None, "mp"), P("mp", None),
        ),
        out_specs=P("dp", "mp", None),
        check_vma=False,
    )
```
